512 devices in a mesh: ta: 64 (over y, x, core), gz: 8 (over z).
Axes of the slice: x: 4, y: 8, z: 8, core: 2. Of those that a mesh axis runs over, the one named last changes fastest.
Arguments:
- time_links: float32 [2, 3, 3, 128, 32, 256], P(None, None, None, 'ta', 'gz'), may hold values from -1 to 1, as said below
- space_links: float32 [3, 2, 3, 3, 128, 32, 256], P(None, None, None, None, 'ta', 'gz'), may hold values from -1 to 1, as said below
Outputs:
- gauge: float32 [2, 3, 3, 128, 32, 256], P(None, None, None, 'ta', 'gz')
- links_fixed: float32 [3, 2, 3, 3, 128, 32, 256], P(None, None, None, None, 'ta', 'gz')
- action_profile: float32 [128, 32], P('ta', 'gz')
- action_mean: float32 [], replicated
The draws below stay inside these ranges and needn't reach their ends.
Inputs may be any that keep to these rules, and one draw needn't show every extreme that they name: `time_links`: every 3 x 3 complex matrix is unitary up to float32 rounding. `space_links`: every 3 x 3 complex matrix is unitary up to float32 rounding.
All inputs are finite; a program needn't handle non-finite values.
Results may differ from the reference program's by a relative error of at most 0.00024.
Values sent between devices are 32-bit elements; how exact they have to be, the bound alone decides.
A program may use at most 64 MiB of HBM per device.

```python
import jax
import jax.numpy as jnp
from jax import lax

X = 16
Y = 16
NT = 128
NZ = 32


def matrix_product(first_pair, second_pair):
    first_real, first_imag = first_pair
    second_real, second_imag = second_pair
    real_part = jnp.sum(first_real[:, :, None] * second_real[None] - first_imag[:, :, None] * second_imag[None], axis=1)
    imag_part = jnp.sum(first_real[:, :, None] * second_imag[None] + first_imag[:, :, None] * second_real[None], axis=1)
    return (real_part, imag_part)


def embedded_block(first_row, second_row, theta, phi, psi):
    ones = jnp.ones_like(theta)
    zeros = jnp.zeros_like(theta)
    real_rows = [[ones if row == col else zeros for col in range(3)] for row in range(3)]
    imag_rows = [[zeros for col in range(3)] for row in range(3)]
    cosine = jnp.cos(theta)
    sine = jnp.sin(theta)
    real_rows[first_row][first_row] = cosine * jnp.cos(phi)
    imag_rows[first_row][first_row] = cosine * jnp.sin(phi)
    real_rows[first_row][second_row] = sine * jnp.cos(psi)
    imag_rows[first_row][second_row] = sine * jnp.sin(psi)
    real_rows[second_row][first_row] = -sine * jnp.cos(psi)
    imag_rows[second_row][first_row] = sine * jnp.sin(psi)
    real_rows[second_row][second_row] = cosine * jnp.cos(phi)
    imag_rows[second_row][second_row] = -cosine * jnp.sin(phi)
    real_part = jnp.stack([jnp.stack(row_list) for row_list in real_rows])
    imag_part = jnp.stack([jnp.stack(row_list) for row_list in imag_rows])
    return (real_part, imag_part)


def unitary_from_angles(angles):
    result = embedded_block(0, 1, angles[0], angles[1], angles[2])
    result = matrix_product(result, embedded_block(0, 2, angles[3], angles[4], angles[5]))
    result = matrix_product(result, embedded_block(1, 2, angles[6], angles[7], angles[8]))
    return jnp.stack([result[0], result[1]])


def draw_time_links(key, part):
    shape_all = (9, NT, NZ, X * Y)
    angles = 1.5 * jax.random.normal(key, shape_all, jnp.float32)
    return unitary_from_angles(angles)


def draw_space_links(key, part):
    shape_all = (3, 9, NT, NZ, X * Y)
    noise_key = jax.random.fold_in(key, 11)
    slice_key = jax.random.fold_in(key, 23)
    plane_key = jax.random.fold_in(key, 37)
    time_frac = (jnp.arange(NT, dtype=jnp.float32) / max(NT - 1, 1))[:, None, None]
    z_frac = (jnp.arange(NZ, dtype=jnp.float32) / max(NZ - 1, 1))[None, :, None]
    slice_factor = jnp.exp(jax.random.uniform(slice_key, (NT,), jnp.float32, -0.35, 0.35))[:, None, None]
    plane_factor = jnp.exp(jax.random.uniform(plane_key, (NZ,), jnp.float32, -0.2, 0.2))[None, :, None]
    wave = 1.0 + 0.3 * jnp.cos(6.2831853 * 3.0 * time_frac + 0.7)
    noise = jax.random.normal(noise_key, shape_all, jnp.float32)
    rise = (1.0 + z_frac) * jnp.sqrt(1.0 + 0.5 * time_frac)
    amplitude = 0.3 * rise * slice_factor * plane_factor * wave
    directions = []
    for direction in range(3):
        directions.append(unitary_from_angles(amplitude * noise[direction]))
    return jnp.stack(directions)


def setup_inputs(seed: int = 0) -> dict:
    seeds = jax.random.split(jax.random.key(seed), 3)
    return {
        "time_links": draw_time_links(jax.random.fold_in(seeds[2], 71), 0),
        "space_links": draw_space_links(jax.random.fold_in(seeds[2], 71), 0),
    }


def complex_product(first_pair, second_pair):
    first_real, first_imag = first_pair
    second_real, second_imag = second_pair
    real_part = jnp.sum(first_real[:, :, None] * second_real[None] - first_imag[:, :, None] * second_imag[None], axis=1)
    imag_part = jnp.sum(first_real[:, :, None] * second_imag[None] + first_imag[:, :, None] * second_real[None], axis=1)
    return real_part, imag_part


def dagger(matrix_pair):
    return jnp.swapaxes(matrix_pair[0], 0, 1), -jnp.swapaxes(matrix_pair[1], 0, 1)


def plane_step(matrix_pair, direction):
    def shifted(values):
        leading = values.shape[:-1]
        lattice_grid = values.reshape(leading + (X, Y))
        lattice_grid = jnp.roll(lattice_grid, -1, axis=lattice_grid.ndim - 2 + direction)
        return lattice_grid.reshape(leading + (X * Y,))
    return shifted(matrix_pair[0]), shifted(matrix_pair[1])


def roll_upward(matrix_pair):
    return jnp.roll(matrix_pair[0], -1, axis=-2), jnp.roll(matrix_pair[1], -1, axis=-2)


def plaquette_density(link_set, forward_x, forward_y):
    forward_z = [forward_x, forward_y]
    terms = []
    for first_dir, second_dir in ((0, 1), (0, 2), (1, 2)):
        along_first = link_set[first_dir]
        along_second = link_set[second_dir]
        second_moved = plane_step(along_second, first_dir)
        if second_dir < 2:
            first_moved = plane_step(along_first, second_dir)
        else:
            first_moved = forward_z[first_dir]
        loop_matrix = complex_product(complex_product(along_first, second_moved),
                                      complex_product(dagger(first_moved), dagger(along_second)))
        trace_real = loop_matrix[0][0, 0] + loop_matrix[0][1, 1] + loop_matrix[0][2, 2]
        terms.append(1.0 - trace_real / 3.0)
    return terms[0] + terms[1] + terms[2]


def reference(time_links, space_links):
    unit_real = jnp.broadcast_to(jnp.eye(3, dtype=jnp.float32)[:, :, None, None], (3, 3, NZ, X * Y))
    start_pair = (unit_real, jnp.zeros_like(unit_real))

    def advance(carry_pair, link_block):
        return complex_product(carry_pair, (link_block[0], link_block[1])), jnp.stack(carry_pair)

    unused_final, gauge_steps = lax.scan(advance, start_pair, jnp.moveaxis(time_links, 3, 0))
    gauge = jnp.moveaxis(gauge_steps, 0, 3)
    gauge_pair = (gauge[0], gauge[1])
    fixed = []
    for direction in range(3):
        link_pair = (space_links[direction, 0], space_links[direction, 1])
        if direction < 2:
            ahead = plane_step(gauge_pair, direction)
        else:
            ahead = roll_upward(gauge_pair)
        fixed.append(complex_product(complex_product(gauge_pair, link_pair), dagger(ahead)))
    links_fixed = jnp.stack([jnp.stack(pair) for pair in fixed])
    density = plaquette_density(fixed, roll_upward(fixed[0]), roll_upward(fixed[1]))
    action_profile = jnp.mean(density, axis=-1) / 3.0
    action_mean = jnp.mean(action_profile)
    return gauge, links_fixed, action_profile, action_mean
```

```python
import jax
import jax.numpy as jnp
from jax import lax
from jax.experimental import pallas as pl
from jax.experimental.pallas import tpu as pltpu
from jax.sharding import PartitionSpec as P

ROWS = 8
LANES = 128
Y = 16
PLANES = 4
HALO_ROWS = (3, 7)
MESH = pl.DeviceIdType.MESH
F32 = jnp.float32


def mul(a, b):
    ar, ai = a
    br, bi = b
    re = im = None
    for k in range(3):
        xr, xi = ar[:, k][:, None], ai[:, k][:, None]
        yr, yi = br[k][None], bi[k][None]
        r = xr * yr - xi * yi
        i = xr * yi + xi * yr
        re, im = (r, i) if re is None else (re + r, im + i)
    return re, im


def mul_dagger(a, b):
    ar, ai = a
    br, bi = b
    re = im = None
    for k in range(3):
        xr, xi = ar[:, k][:, None], ai[:, k][:, None]
        yr, yi = br[:, k][None], bi[:, k][None]
        r = xr * yr + xi * yi
        i = xi * yr - xr * yi
        re, im = (r, i) if re is None else (re + r, im + i)
    return re, im


def both(fn, pair):
    return fn(pair[0]), fn(pair[1])


def rows_of(shape):
    return lax.broadcasted_iota(jnp.int32, shape, len(shape) - 2)


def lanes_of(shape):
    return lax.broadcasted_iota(jnp.int32, shape, len(shape) - 1)


def pick(mask, a, b):
    return jnp.where(mask, a[0], b[0]), jnp.where(mask, a[1], b[1])


def ahead_x(pair):
    def shift(v):
        near = pltpu.roll(v, LANES - Y, v.ndim - 1)
        far = pltpu.roll(near, PLANES, v.ndim - 2)
        return jnp.where(lanes_of(v.shape) >= LANES - Y, far, near)

    return both(shift, pair)


def ahead_y(pair):
    def shift(v):
        near = pltpu.roll(v, LANES - 1, v.ndim - 1)
        wrap = pltpu.roll(v, Y - 1, v.ndim - 1)
        return jnp.where(lanes_of(v.shape) % Y == Y - 1, wrap, near)

    return both(shift, pair)


def ahead_z(pair, halo):
    def shift(v, h):
        near = pltpu.roll(v, ROWS - 1, v.ndim - 2)
        return jnp.where(rows_of(v.shape) % PLANES == PLANES - 1, h, near)

    return shift(pair[0], halo[0]), shift(pair[1], halo[1])


def or_unit(mask, pair):
    re, im = pair
    return (
        jnp.stack(
            [
                jnp.stack([jnp.where(mask, re[i, j], 1.0 if i == j else 0.0) for j in range(3)])
                for i in range(3)
            ]
        ),
        jnp.where(mask, im, 0.0),
    )


def row_of(ref, row):
    return ref.at[:, :, :, pl.ds(row, 1), :]


def load(ref):
    return ref[0], ref[1]


def kernel(
    time_ref, space_ref, gauge_ref, fixed_ref, profile_ref, mean_ref,
    tl, sl, total, scanned, spread, in1, in2, carry, carry_halo, time_halo, space_halo,
    g_out, v_out, part, part_in,
    load_sem, store_sem, halo_send, halo_recv,
    send1, recv1, send2, recv2, send3, recv3, send4, recv4, send_part, recv_part,
):
    me = lax.axis_index("ta")
    z = lax.axis_index("gz")
    group, member = me // ROWS, me % ROWS
    below = (z + 7) % 8

    def in_row(k):
        return group * ROWS + (member + k) % ROWS, z

    def in_column(k):
        return (group + k) % ROWS * ROWS + member, z

    def in_height(k):
        return me, (z + k) % ROWS

    barrier = pltpu.get_barrier_semaphore()
    for k in range(1, ROWS):
        for device in (in_row(k), in_column(k), in_height(k)):
            pl.semaphore_signal(barrier, inc=1, device_id=device, device_id_type=MESH)

    loads = []
    for c in range(2):
        loads.append(pltpu.make_async_copy(
            time_ref.at[:, :, :, :, :, pl.ds(c * LANES, LANES)],
            tl.at[:, :, :, :, pl.ds(c * PLANES, PLANES), :],
            load_sem.at[c],
        ))
    for c in range(2):
        loads.append(pltpu.make_async_copy(
            space_ref.at[:, :, :, :, :, :, pl.ds(c * LANES, LANES)],
            sl.at[:, :, :, :, :, pl.ds(c * PLANES, PLANES), :],
            load_sem.at[2 + c],
        ))
    for copy in loads:
        copy.start()
    loads[0].wait()
    loads[1].wait()

    def time_link(t):
        return tl[0, :, :, t], tl[1, :, :, t]

    def space_link(mu, t):
        return sl[mu, 0, :, :, t], sl[mu, 1, :, :, t]

    prod = mul(time_link(0), time_link(1))
    total[0], total[1] = prod
    pl.semaphore_wait(barrier, 3 * (ROWS - 1))

    def remote(src, dst, send, recv, device):
        return pltpu.make_async_remote_copy(
            src_ref=src, dst_ref=dst, send_sem=send, recv_sem=recv,
            device_id=device, device_id_type=MESH,
        )

    first = []
    for k in range(1, ROWS):
        first.append(remote(
            row_of(total, (member + k) % ROWS), row_of(in1, member),
            send1.at[k], recv1.at[k], in_row(k),
        ))
    for copy in first:
        copy.start()

    loads[2].wait()
    loads[3].wait()
    halos = []
    for c in range(2):
        for mu in range(2):
            halos.append(remote(
                sl.at[mu, :, :, :, :, pl.ds(c * PLANES, 1), :],
                space_halo.at[mu, :, :, :, :, pl.ds(HALO_ROWS[c], 1), :],
                halo_send.at[c * 2 + mu], halo_recv.at[c * 2 + mu], (me, below),
            ))
    for c in range(2):
        halos.append(remote(
            tl.at[:, :, :, 0, pl.ds(c * PLANES, 1), :],
            time_halo.at[:, :, :, pl.ds(HALO_ROWS[c], 1), :],
            halo_send.at[4 + c], halo_recv.at[4 + c], (me, below),
        ))
    for copy in halos:
        copy.start()

    rows = rows_of((ROWS, LANES))
    for copy in first:
        copy.wait_recv()
    scan = pick(rows == member, load(total), load(in1))
    for s in (1, 2, 4):
        earlier = both(lambda v: pltpu.roll(v, s, 2), scan)
        scan = pick(rows >= s, mul(earlier, scan), scan)
    scanned[0], scanned[1] = scan

    second = []
    for k in range(1, ROWS):
        second.append(remote(
            row_of(scanned, ROWS - 1), row_of(in2, group),
            send2.at[k], recv2.at[k], in_column(k),
        ))
    for copy in second:
        copy.start()

    for copy in halos:
        copy.wait_recv()
    sites = jnp.zeros((ROWS, LANES), F32)
    lanes = lanes_of((ROWS, LANES))
    for t in range(2):
        density = jnp.zeros((ROWS, LANES), F32)
        for mu, nu in ((0, 1), (0, 2), (1, 2)):
            along_mu, along_nu = space_link(mu, t), space_link(nu, t)
            nu_moved = ahead_x(along_nu) if mu == 0 else ahead_y(along_nu)
            if nu == 1:
                mu_moved = ahead_y(along_mu)
            else:
                mu_moved = ahead_z(
                    along_mu, (space_halo[mu, 0, :, :, t], space_halo[mu, 1, :, :, t])
                )
            there, back = mul(along_mu, nu_moved), mul(along_nu, mu_moved)
            trace = jnp.sum(there[0] * back[0] + there[1] * back[1], axis=(0, 1))
            density = density + (1.0 - trace / 3.0)
        of_row = jnp.sum(density, axis=1, keepdims=True)
        spots = jnp.where(lanes == rows % PLANES, of_row, 0.0)
        profile = jnp.sum(spots, axis=0, keepdims=True) * (1.0 / (3 * 2 * LANES))
        profile_ref[t : t + 1, :] = profile[:, :PLANES]
        sites = sites + density
    part[0] = jnp.broadcast_to(jnp.sum(sites, axis=0, keepdims=True), (ROWS, LANES))

    def add_up(stage, place, partner):
        copies = []
        for k in range(1, ROWS):
            copies.append(remote(
                part.at[stage, pl.ds(0, 1), :], part_in.at[stage, pl.ds(place, 1), :],
                send_part.at[stage, k], recv_part.at[stage, k], partner(k),
            ))
        for copy in copies:
            copy.start()
        return copies

    def added(stage, place, copies):
        for copy in copies:
            copy.wait_recv()
        parts = jnp.where(rows == place, part[stage], part_in[stage])
        return jnp.broadcast_to(jnp.sum(parts, axis=0, keepdims=True), (ROWS, LANES))

    stage0 = add_up(0, member, in_row)

    for copy in second:
        copy.wait_recv()
    before = or_unit(rows < group, load(in2))
    for s in (1, 2, 4):
        before = mul(before, both(lambda v: pltpu.roll(v, ROWS - s, 2), before))
    before = both(lambda v: jnp.broadcast_to(v[:, :, 0:1], v.shape), before)
    inside = both(lambda v: pltpu.roll(v, 1, 2), scan)
    start = mul(before, or_unit(rows >= 1, inside))
    spread[0], spread[1] = start

    third = []
    for k in range(1, ROWS):
        third.append(remote(
            row_of(spread, (member + k) % ROWS), row_of(carry, member),
            send3.at[k], recv3.at[k], in_row(k),
        ))
    for copy in third:
        copy.start()
    lowest = member % PLANES == 0
    for k in range(ROWS):
        @pl.when(lowest)
        def _(k=k):
            remote(
                row_of(spread, k), row_of(carry_halo, member + PLANES - 1),
                send4.at[k], recv4.at[member // PLANES], (group * ROWS + k, below),
            ).start()

    part[1] = added(0, member, stage0)
    stage1 = add_up(1, z, in_height)

    for copy in third:
        copy.wait_recv()
    g0 = pick(rows == member, load(spread), load(carry))
    g1 = mul(g0, time_link(0))
    g = (g0, g1)
    for t in range(2):
        g_out[0, :, :, t], g_out[1, :, :, t] = g[t]

    stores = []

    def store(src, dst):
        for c in range(2):
            copy = pltpu.make_async_copy(
                src(pl.ds(c * PLANES, PLANES)), dst(pl.ds(c * LANES, LANES)),
                store_sem.at[len(stores)],
            )
            copy.start()
            stores.append(copy)

    store(lambda q: g_out.at[:, :, :, :, q, :], lambda q: gauge_ref.at[:, :, :, :, :, q])

    def fix(mu, t, ahead):
        v = mul_dagger(mul(g[t], space_link(mu, t)), ahead)
        v_out[mu, 0, :, :, t], v_out[mu, 1, :, :, t] = v

    def store_fixed(mu):
        store(
            lambda q: v_out.at[mu, :, :, :, :, q, :],
            lambda q: fixed_ref.at[mu, :, :, :, :, :, q],
        )

    for t in range(2):
        fix(0, t, ahead_x(g[t]))
    store_fixed(0)
    for t in range(2):
        fix(1, t, ahead_y(g[t]))
    store_fixed(1)
    for c in range(2):
        remote(
            row_of(spread, 0), row_of(carry_halo, HALO_ROWS[c]),
            send4.at[c], recv4.at[c], (me, below),
        ).wait_recv()
    g0z = ahead_z(g0, load(carry_halo))
    g1z = mul(g0z, ahead_z(time_link(0), load(time_halo)))
    for t, ahead in ((0, g0z), (1, g1z)):
        fix(2, t, ahead)
    store_fixed(2)

    part[2] = added(1, z, stage1)
    stage2 = add_up(2, group, in_column)
    whole = added(2, group, stage2)
    mean = jnp.sum(whole[0:1], axis=1, keepdims=True)
    mean_ref[...] = mean * (1.0 / (3 * 2 * LANES * 4096))

    for copy in stores:
        copy.wait()
    for copy in first + halos + second + stage0 + third + stage1 + stage2:
        copy.wait_send()
    for k in range(ROWS):
        @pl.when(lowest)
        def _(k=k):
            remote(
                row_of(spread, k), row_of(carry_halo, member + PLANES - 1),
                send4.at[k], recv4.at[member // PLANES], (group * ROWS + k, below),
            ).wait_send()


def on_device(time_links, space_links):
    pair = (2, 3, 3, ROWS, LANES)
    dma = pltpu.SemaphoreType.DMA
    gauge, fixed, profile, mean = pl.pallas_call(
        kernel,
        out_shape=(
            jax.ShapeDtypeStruct(time_links.shape, F32),
            jax.ShapeDtypeStruct(space_links.shape, F32),
            jax.ShapeDtypeStruct((2, PLANES), F32),
            jax.ShapeDtypeStruct((1, 1), F32),
        ),
        in_specs=[pl.BlockSpec(memory_space=pl.ANY)] * 2,
        out_specs=(
            pl.BlockSpec(memory_space=pl.ANY),
            pl.BlockSpec(memory_space=pl.ANY),
            pl.BlockSpec(memory_space=pltpu.VMEM),
            pl.BlockSpec(memory_space=pltpu.VMEM),
        ),
        scratch_shapes=[
            pltpu.VMEM((2, 3, 3, 2, ROWS, LANES), F32),
            pltpu.VMEM((3, 2, 3, 3, 2, ROWS, LANES), F32),
            pltpu.VMEM(pair, F32),
            pltpu.VMEM(pair, F32),
            pltpu.VMEM(pair, F32),
            pltpu.VMEM(pair, F32),
            pltpu.VMEM(pair, F32),
            pltpu.VMEM(pair, F32),
            pltpu.VMEM(pair, F32),
            pltpu.VMEM(pair, F32),
            pltpu.VMEM((2, 2, 3, 3, 2, ROWS, LANES), F32),
            pltpu.VMEM((2, 3, 3, 2, ROWS, LANES), F32),
            pltpu.VMEM((3, 2, 3, 3, 2, ROWS, LANES), F32),
            pltpu.VMEM((3, ROWS, LANES), F32),
            pltpu.VMEM((3, ROWS, LANES), F32),
            dma((4,)), dma((8,)), dma((6,)), dma((6,)),
            dma((ROWS,)), dma((ROWS,)), dma((ROWS,)), dma((ROWS,)),
            dma((ROWS,)), dma((ROWS,)), dma((ROWS,)), dma((2,)),
            dma((3, ROWS)), dma((3, ROWS)),
        ],
        compiler_params=pltpu.CompilerParams(collective_id=0, has_side_effects=True),
    )(time_links, space_links)
    return gauge, fixed, profile, mean.reshape(())


def solution(mesh):
    placed = (P(None, None, None, "ta", "gz", None), P(None, None, None, None, "ta", "gz", None))
    return jax.shard_map(
        on_device,
        mesh=mesh,
        in_specs=placed,
        out_specs=(*placed, P("ta", "gz"), P()),
        check_vma=False,
    )
```

```python
import jax
import jax.numpy as jnp
from jax import lax
from jax.experimental import pallas as pl
from jax.experimental.pallas import tpu as pltpu
from jax.sharding import PartitionSpec as P

ROWS = 8
LANES = 128
Y = 16
PLANES = 4
HALO_ROWS = (3, 7)
EARLY = 4
DEPTH = 8
MESH = pl.DeviceIdType.MESH
F32 = jnp.float32


def mul(a, b):
    ar, ai = a
    br, bi = b
    re = im = None
    for k in range(3):
        xr, xi = ar[:, k][:, None], ai[:, k][:, None]
        yr, yi = br[k][None], bi[k][None]
        r = xr * yr - xi * yi
        i = xr * yi + xi * yr
        re, im = (r, i) if re is None else (re + r, im + i)
    return re, im


def mul_dagger(a, b):
    ar, ai = a
    br, bi = b
    re = im = None
    for k in range(3):
        xr, xi = ar[:, k][:, None], ai[:, k][:, None]
        yr, yi = br[:, k][None], bi[:, k][None]
        r = xr * yr + xi * yi
        i = xi * yr - xr * yi
        re, im = (r, i) if re is None else (re + r, im + i)
    return re, im


def dagger_mul(a, b):
    ar, ai = a
    br, bi = b
    re = im = None
    for k in range(3):
        xr, xi = ar[k][:, None], ai[k][:, None]
        yr, yi = br[k][None], bi[k][None]
        r = xr * yr + xi * yi
        i = xr * yi - xi * yr
        re, im = (r, i) if re is None else (re + r, im + i)
    return re, im


def overlap(a, b):
    return jnp.sum(a[0] * b[0] + a[1] * b[1], axis=(0, 1))


def both(fn, pair):
    return fn(pair[0]), fn(pair[1])


def rows_of(shape):
    return lax.broadcasted_iota(jnp.int32, shape, len(shape) - 2)


def lanes_of(shape):
    return lax.broadcasted_iota(jnp.int32, shape, len(shape) - 1)


def pick(mask, a, b):
    return jnp.where(mask, a[0], b[0]), jnp.where(mask, a[1], b[1])


def ahead_x(pair):
    def shift(v):
        near = pltpu.roll(v, LANES - Y, v.ndim - 1)
        far = pltpu.roll(near, PLANES, v.ndim - 2)
        return jnp.where(lanes_of(v.shape) >= LANES - Y, far, near)

    return both(shift, pair)


def ahead_y(pair):
    def shift(v):
        near = pltpu.roll(v, LANES - 1, v.ndim - 1)
        wrap = pltpu.roll(v, Y - 1, v.ndim - 1)
        return jnp.where(lanes_of(v.shape) % Y == Y - 1, wrap, near)

    return both(shift, pair)


def up_z(pair):
    return both(lambda v: pltpu.roll(v, ROWS - 1, v.ndim - 2), pair)


def ahead_z(pair, halo):
    top = rows_of((ROWS, LANES)) % PLANES == PLANES - 1
    return pick(top, halo, up_z(pair))


def or_unit(mask, pair):
    re, im = pair
    return (
        jnp.stack(
            [
                jnp.stack([jnp.where(mask, re[i, j], 1.0 if i == j else 0.0) for j in range(3)])
                for i in range(3)
            ]
        ),
        jnp.where(mask, im, 0.0),
    )


def row_of(ref, row):
    return ref.at[:, :, :, pl.ds(row, 1), :]


def load(ref):
    return ref[0], ref[1]


def kernel(
    time_ref, space_ref, g_out, v_out, profile_ref, mean_ref,
    tl, sl, total, scanned, spread, in1, in2, carry, carry_halo, time_halo, space_halo,
    around, part, part_row, part_all, part_back,
    load_sem, halo_send, halo_recv,
    send1, recv1, send2, recv2, send3, recv3, send4, recv4,
    send_row, recv_row, send_all, recv_all, send_back, recv_back,
):
    me = lax.axis_index("ta")
    z = lax.axis_index("gz")
    group, member = me // ROWS, me % ROWS
    below, above = (z + DEPTH - 1) % DEPTH, (z + 1) % DEPTH
    early = z < EARLY

    def in_row(k):
        return group * ROWS + (member + k) % ROWS, z

    def in_column(k, height=z):
        return (group + k) % ROWS * ROWS + member, height

    space_loads, time_loads = [], []
    for c in range(2):
        space_loads.append(pltpu.make_async_copy(
            space_ref.at[:, :, :, :, :, :, pl.ds(c * LANES, LANES)],
            sl.at[:, :, :, :, :, pl.ds(c * PLANES, PLANES), :],
            load_sem.at[c],
        ))
    for c in range(2):
        time_loads.append(pltpu.make_async_copy(
            time_ref.at[:, :, :, :, :, pl.ds(c * LANES, LANES)],
            tl.at[:, :, :, :, pl.ds(c * PLANES, PLANES), :],
            load_sem.at[2 + c],
        ))
    for copy in space_loads + time_loads:
        copy.start()

    barrier = pltpu.get_barrier_semaphore()

    def greet(device):
        pl.semaphore_signal(barrier, inc=1, device_id=device, device_id_type=MESH)

    for k in range(1, ROWS):
        greet(in_row(k))

    @pl.when(early)
    def _():
        for k in range(1, DEPTH):
            greet((me, (z + k) % DEPTH))

        def to_column(k, carried):
            for height in range(DEPTH):
                greet(in_column(k, height))
            return carried

        lax.fori_loop(1, ROWS, to_column, 0)

    @pl.when(jnp.logical_not(early))
    def _():
        for k in range(1, ROWS):
            greet(in_column(k))
        greet((me, above))

    def time_link(t):
        return tl[0, :, :, t], tl[1, :, :, t]

    def space_link(mu, t):
        return sl[mu, 0, :, :, t], sl[mu, 1, :, :, t]

    def remote(src, dst, send, recv, device):
        return pltpu.make_async_remote_copy(
            src_ref=src, dst_ref=dst, send_sem=send, recv_sem=recv,
            device_id=device, device_id_type=MESH,
        )

    for copy in space_loads:
        copy.wait()
    late_below = jnp.logical_or(z == 0, z > EARLY).astype(jnp.int32)
    of_column = jnp.where(early, EARLY * ROWS - 1, EARLY * ROWS + ROWS - 1)
    pl.semaphore_wait(barrier, ROWS - 1 + of_column + late_below)

    halos = []
    for mu in range(2):
        for c in range(2):
            halos.append(remote(
                sl.at[mu, :, :, :, :, pl.ds(c * PLANES, 1), :],
                space_halo.at[mu, :, :, :, :, pl.ds(HALO_ROWS[c], 1), :],
                halo_send.at[c * 2 + mu], halo_recv.at[c * 2 + mu], (me, below),
            ))
    for copy in halos:
        copy.start()

    for copy in time_loads:
        copy.wait()
    prod = mul(time_link(0), time_link(1))
    total[0], total[1] = prod

    first = []
    for k in range(1, ROWS):
        first.append(remote(
            row_of(total, (member + k) % ROWS), row_of(in1, member),
            send1.at[k], recv1.at[k], in_row(k),
        ))
    for copy in first:
        copy.start()
    time_halos = []
    for c in range(2):
        time_halos.append(remote(
            tl.at[:, :, :, 0, pl.ds(c * PLANES, 1), :],
            time_halo.at[:, :, :, pl.ds(HALO_ROWS[c], 1), :],
            halo_send.at[4 + c], halo_recv.at[4 + c], (me, below),
        ))
    for copy in time_halos:
        copy.start()

    rows = rows_of((ROWS, LANES))
    lanes = lanes_of((ROWS, LANES))
    top = rows % PLANES == PLANES - 1
    traces = []
    for t in range(2):
        ux, uy, uz = (space_link(mu, t) for mu in range(3))
        trace = overlap(mul(ux, ahead_x(uy)), mul(uy, ahead_y(ux)))
        for mu, along, ahead in ((0, ux, ahead_x), (1, uy, ahead_y)):
            rest = dagger_mul(uz, mul(along, ahead(uz)))
            around[mu, 0, :, :, t], around[mu, 1, :, :, t] = rest
            trace = trace + jnp.where(top, 0.0, overlap(rest, up_z(along)))
        traces.append(trace)
    for copy in halos:
        copy.wait_recv()
    densities = []
    for t in range(2):
        trace = traces[t]
        for mu in range(2):
            rest = around[mu, 0, :, :, t], around[mu, 1, :, :, t]
            beyond = space_halo[mu, 0, :, :, t], space_halo[mu, 1, :, :, t]
            trace = trace + jnp.where(top, overlap(rest, beyond), 0.0)
        densities.append(3.0 - trace * (1.0 / 3.0))

    def spread_sum(v):
        return jnp.broadcast_to(jnp.sum(v, axis=0, keepdims=True), (ROWS, LANES))

    part[0] = spread_sum(densities[0] + densities[1])
    row_parts = []
    for k in range(1, ROWS):
        row_parts.append(remote(
            part.at[0, pl.ds(0, 1), :], part_row.at[pl.ds(member, 1), :],
            send_row.at[k], recv_row.at[k], in_row(k),
        ))
    for copy in row_parts:
        copy.start()

    for t in range(2):
        of_row = jnp.sum(densities[t], axis=1, keepdims=True)
        spots = jnp.where(lanes == rows % PLANES, of_row, 0.0)
        profile = jnp.sum(spots, axis=0, keepdims=True) * (1.0 / (3 * 2 * LANES))
        profile_ref[t : t + 1, :] = profile[:, :PLANES]

    for copy in first:
        copy.wait_recv()
    scan = pick(rows == member, load(total), load(in1))
    for s in (1, 2, 4):
        earlier = both(lambda v: pltpu.roll(v, s, 2), scan)
        scan = pick(rows >= s, mul(earlier, scan), scan)
    scanned[0], scanned[1] = scan

    def to_later(k):
        return remote(
            row_of(scanned, ROWS - 1), row_of(in2, group),
            send2.at[k], recv2.at[k], in_column(k),
        )

    for k in range(ROWS - 1, 0, -1):
        @pl.when(group + k < ROWS)
        def _(k=k):
            to_later(k).start()

    for copy in row_parts:
        copy.wait_recv()
    part[1] = spread_sum(jnp.where(rows == member, part[0], part_row[...]))

    def to_early(k, height):
        return remote(
            part.at[1, pl.ds(0, 1), :], part_all.at[group, pl.ds(z, 1), :],
            send_all.at[k, height], recv_all.at[k, z], in_column(k, height),
        )

    def each_early(act):
        for height in range(EARLY):
            @pl.when(z != height)
            def _(height=height):
                act(to_early(0, height))

        def at(k, carried):
            for height in range(EARLY):
                act(to_early(k, height))
            return carried

        lax.fori_loop(1, ROWS, at, 0)

    each_early(lambda copy: copy.start())

    inside = or_unit(rows >= 1, both(lambda v: pltpu.roll(v, 1, 2), scan))
    for k in range(1, ROWS):
        @pl.when(group >= k)
        def _(k=k):
            to_later(k).wait_recv()
    before = or_unit(rows < group, load(in2))
    for s in (1, 2, 4):
        before = mul(before, both(lambda v: pltpu.roll(v, ROWS - s, 2), before))
    before = both(lambda v: jnp.broadcast_to(v[:, :, 0:1], v.shape), before)
    spread[0], spread[1] = mul(before, inside)

    third = []
    for k in range(1, ROWS):
        third.append(remote(
            row_of(spread, (member + k) % ROWS), row_of(carry, member),
            send3.at[k], recv3.at[k], in_row(k),
        ))
    for copy in third:
        copy.start()
    lowest = member % PLANES == 0

    def to_below(k):
        return remote(
            row_of(spread, k), row_of(carry_halo, member + PLANES - 1),
            send4.at[k], recv4.at[member // PLANES], (group * ROWS + k, below),
        )

    for k in range(ROWS):
        @pl.when(lowest)
        def _(k=k):
            to_below(k).start()

    for copy in third:
        copy.wait_recv()
    g0 = pick(rows == member, load(spread), load(carry))
    g1 = mul(g0, time_link(0))
    g = (g0, g1)
    for t in range(2):
        g_out[0, :, :, t], g_out[1, :, :, t] = g[t]

    def fix(mu, t, ahead):
        v = mul_dagger(mul(g[t], space_link(mu, t)), ahead)
        v_out[mu, 0, :, :, t], v_out[mu, 1, :, :, t] = v

    for t in range(2):
        fix(0, t, ahead_x(g[t]))
    for t in range(2):
        fix(1, t, ahead_y(g[t]))
    for copy in time_halos:
        copy.wait_recv()
    for c in range(2):
        remote(
            row_of(spread, 0), row_of(carry_halo, HALO_ROWS[c]),
            send4.at[c], recv4.at[c], (me, below),
        ).wait_recv()
    g0z = ahead_z(g0, load(carry_halo))
    g1z = mul(g0z, ahead_z(time_link(0), load(time_halo)))
    for t, ahead in ((0, g0z), (1, g1z)):
        fix(2, t, ahead)

    def to_late():
        return remote(
            part.at[2], part_back, send_back.at[0], recv_back.at[0], (me, (z + EARLY) % DEPTH)
        )

    def write_mean(sites):
        mean = jnp.sum(sites[0:1], axis=1, keepdims=True)
        mean_ref[...] = mean * (1.0 / (3 * 2 * LANES * 4096))

    @pl.when(early)
    def _():
        for height in range(DEPTH):
            @pl.when(z != height)
            def _(height=height):
                remote(
                    part.at[1, pl.ds(0, 1), :], part_all.at[0, pl.ds(0, 1), :],
                    send_all.at[0, 0], recv_all.at[0, height], (me, below),
                ).wait_recv()

        def one(k, carried):
            for height in range(DEPTH):
                remote(
                    part.at[1, pl.ds(0, 1), :], part_all.at[0, pl.ds(0, 1), :],
                    send_all.at[0, 0], recv_all.at[k, height], (me, below),
                ).wait_recv()
            return carried

        lax.fori_loop(1, ROWS, one, 0)
        parts = None
        for k in range(ROWS):
            mine = jnp.logical_and(rows == z, group == k)
            got = jnp.where(mine, part[1], part_all[k])
            parts = got if parts is None else parts + got
        whole = spread_sum(parts)
        part[2] = whole
        to_late().start()
        write_mean(whole)
        to_late().wait_send()

    @pl.when(jnp.logical_not(early))
    def _():
        to_late().wait_recv()
        write_mean(part_back[...])

    for copy in halos + first + time_halos + row_parts + third:
        copy.wait_send()
    for k in range(1, ROWS):
        @pl.when(group + k < ROWS)
        def _(k=k):
            to_later(k).wait_send()
    each_early(lambda copy: copy.wait_send())
    for k in range(ROWS):
        @pl.when(lowest)
        def _(k=k):
            to_below(k).wait_send()


def write_out(g_out, v_out, profile, mean, gauge_ref, fixed_ref, profile_ref, mean_ref, sem):
    copies = []
    for c in range(2):
        planes, lanes = pl.ds(c * PLANES, PLANES), pl.ds(c * LANES, LANES)
        for src, dst in (
            (v_out.at[:, :, :, :, :, planes, :], fixed_ref.at[:, :, :, :, :, :, lanes]),
            (g_out.at[:, :, :, :, planes, :], gauge_ref.at[:, :, :, :, :, lanes]),
        ):
            copies.append(pltpu.make_async_copy(src, dst, sem.at[len(copies)]))
    for src, dst in ((profile, profile_ref), (mean, mean_ref)):
        copies.append(pltpu.make_async_copy(src, dst, sem.at[len(copies)]))
    for copy in copies:
        copy.start()
    for copy in copies:
        copy.wait()


def on_device(time_links, space_links):
    pair = (2, 3, 3, ROWS, LANES)
    dma = pltpu.SemaphoreType.DMA
    vmem = pl.BlockSpec(memory_space=pltpu.VMEM)
    anywhere = pl.BlockSpec(memory_space=pl.ANY)
    staged = pl.pallas_call(
        kernel,
        out_shape=(
            pltpu.VMEM((2, 3, 3, 2, ROWS, LANES), F32),
            pltpu.VMEM((3, 2, 3, 3, 2, ROWS, LANES), F32),
            pltpu.VMEM((2, PLANES), F32),
            pltpu.VMEM((1, 1), F32),
        ),
        in_specs=[pl.BlockSpec(memory_space=pltpu.HBM)] * 2,
        out_specs=(vmem,) * 4,
        scratch_shapes=[
            pltpu.VMEM((2, 3, 3, 2, ROWS, LANES), F32),
            pltpu.VMEM((3, 2, 3, 3, 2, ROWS, LANES), F32),
            *[pltpu.VMEM(pair, F32)] * 8,
            pltpu.VMEM((2, 2, 3, 3, 2, ROWS, LANES), F32),
            pltpu.VMEM((2, 2, 3, 3, 2, ROWS, LANES), F32),
            pltpu.VMEM((3, ROWS, LANES), F32),
            pltpu.VMEM((ROWS, LANES), F32),
            pltpu.VMEM((ROWS, DEPTH, LANES), F32),
            pltpu.VMEM((ROWS, LANES), F32),
            dma((4,)), dma((6,)), dma((6,)),
            dma((ROWS,)), dma((ROWS,)), dma((ROWS,)), dma((ROWS,)),
            dma((ROWS,)), dma((ROWS,)), dma((ROWS,)), dma((2,)),
            dma((ROWS,)), dma((ROWS,)), dma((ROWS, EARLY)), dma((ROWS, DEPTH)),
            dma((1,)), dma((1,)),
        ],
        compiler_params=pltpu.CompilerParams(collective_id=0, has_side_effects=True),
    )(time_links, space_links)
    gauge, fixed, profile, mean = pl.pallas_call(
        write_out,
        out_shape=(
            jax.ShapeDtypeStruct(time_links.shape, F32),
            jax.ShapeDtypeStruct(space_links.shape, F32),
            jax.ShapeDtypeStruct((2, PLANES), F32),
            jax.ShapeDtypeStruct((1, 1), F32),
        ),
        in_specs=[vmem] * 4,
        out_specs=(anywhere,) * 4,
        scratch_shapes=[dma((6,))],
        compiler_params=pltpu.CompilerParams(vmem_limit_bytes=4 * 2**20),
    )(*staged)
    return gauge, fixed, profile, mean.reshape(())


def solution(mesh):
    placed = (P(None, None, None, "ta", "gz", None), P(None, None, None, None, "ta", "gz", None))
    return jax.shard_map(
        on_device,
        mesh=mesh,
        in_specs=placed,
        out_specs=(*placed, P("ta", "gz"), P()),
        check_vma=False,
    )
```

```python
import jax
import jax.numpy as jnp
from jax import lax
from jax.experimental import pallas as pl
from jax.experimental.pallas import tpu as pltpu
from jax.sharding import PartitionSpec as P

ROWS = 8
LANES = 128
Y = 16
PLANES = 4
HALO_ROWS = (3, 7)
EARLY = 4
DEPTH = 8
PLANE = 64
SEMAPHORES = 20
MESH = pl.DeviceIdType.MESH
F32 = jnp.float32


def mul(a, b):
    ar, ai = a
    br, bi = b
    re = im = None
    for k in range(3):
        xr, xi = ar[:, k][:, None], ai[:, k][:, None]
        yr, yi = br[k][None], bi[k][None]
        r = xr * yr - xi * yi
        i = xr * yi + xi * yr
        re, im = (r, i) if re is None else (re + r, im + i)
    return re, im


def mul_dagger(a, b):
    ar, ai = a
    br, bi = b
    re = im = None
    for k in range(3):
        xr, xi = ar[:, k][:, None], ai[:, k][:, None]
        yr, yi = br[:, k][None], bi[:, k][None]
        r = xr * yr + xi * yi
        i = xi * yr - xr * yi
        re, im = (r, i) if re is None else (re + r, im + i)
    return re, im


def dagger_mul(a, b):
    ar, ai = a
    br, bi = b
    re = im = None
    for k in range(3):
        xr, xi = ar[k][:, None], ai[k][:, None]
        yr, yi = br[k][None], bi[k][None]
        r = xr * yr + xi * yi
        i = xr * yi - xi * yr
        re, im = (r, i) if re is None else (re + r, im + i)
    return re, im


def overlap(a, b):
    return jnp.sum(a[0] * b[0] + a[1] * b[1], axis=(0, 1))


def both(fn, pair):
    return fn(pair[0]), fn(pair[1])


def rows_of(shape):
    return lax.broadcasted_iota(jnp.int32, shape, len(shape) - 2)


def lanes_of(shape):
    return lax.broadcasted_iota(jnp.int32, shape, len(shape) - 1)


def pick(mask, a, b):
    return jnp.where(mask, a[0], b[0]), jnp.where(mask, a[1], b[1])


def ahead_x(pair):
    def shift(v):
        near = pltpu.roll(v, LANES - Y, v.ndim - 1)
        far = pltpu.roll(near, PLANES, v.ndim - 2)
        return jnp.where(lanes_of(v.shape) >= LANES - Y, far, near)

    return both(shift, pair)


def ahead_y(pair):
    def shift(v):
        near = pltpu.roll(v, LANES - 1, v.ndim - 1)
        wrap = pltpu.roll(v, Y - 1, v.ndim - 1)
        return jnp.where(lanes_of(v.shape) % Y == Y - 1, wrap, near)

    return both(shift, pair)


def up_z(pair):
    return both(lambda v: pltpu.roll(v, ROWS - 1, v.ndim - 2), pair)


def ahead_z(pair, halo):
    top = rows_of((ROWS, LANES)) % PLANES == PLANES - 1
    return pick(top, halo, up_z(pair))


def or_unit(mask, pair):
    re, im = pair
    return (
        jnp.stack(
            [
                jnp.stack([jnp.where(mask, re[i, j], 1.0 if i == j else 0.0) for j in range(3)])
                for i in range(3)
            ]
        ),
        jnp.where(mask, im, 0.0),
    )


def row_of(ref, row):
    return ref.at[:, :, :, pl.ds(row, 1), :]


def rows_in(ref, count):
    return ref.at[:, :, :, pl.ds(0, count), :]


def drain(ref, sem):
    pltpu.make_async_copy(ref, ref, sem).wait()


def load(ref):
    return ref[0], ref[1]


def kernel(
    time_ref, space_ref, g_out, v_out, small,
    tl, sl, total, scanned, spread, in1, in2, carry, carry_halo, time_halo, space_halo,
    around, part, part_z, part_all, part_back,
    sems, near_sem, far_sem, plane_sem,
):
    (
        load_space, load_time, halo_send, halo_recv, time_send, time_recv,
        send1, recv1, send2, recv2, send3, recv3, send4, recv4,
        send_z, recv_z, send_all, recv_all, send_back, recv_back,
    ) = (sems.at[i] for i in range(SEMAPHORES))
    me = lax.axis_index("ta")
    z = lax.axis_index("gz")
    group, member = me // ROWS, me % ROWS
    below, above = (z + DEPTH - 1) % DEPTH, (z + 1) % DEPTH
    early = z < EARLY

    def in_row(k):
        return group * ROWS + (member + k) % ROWS, z

    def in_column(k):
        return (group + k) % ROWS * ROWS + member, z

    space_loads, time_loads = [], []
    for c in range(2):
        space_loads.append(pltpu.make_async_copy(
            space_ref.at[:, :, :, :, :, :, pl.ds(c * LANES, LANES)],
            sl.at[:, :, :, :, :, pl.ds(c * PLANES, PLANES), :],
            load_space,
        ))
    for c in range(2):
        time_loads.append(pltpu.make_async_copy(
            time_ref.at[:, :, :, :, :, pl.ds(c * LANES, LANES)],
            tl.at[:, :, :, :, pl.ds(c * PLANES, PLANES), :],
            load_time,
        ))
    for copy in space_loads + time_loads:
        copy.start()

    barrier = pltpu.get_barrier_semaphore()

    def greet(device):
        pl.semaphore_signal(barrier, inc=1, device_id=device, device_id_type=MESH)

    greet((me, above))
    for k in range(1, ROWS):
        greet(in_row(k))
    for k in (1, ROWS - 1):
        greet(in_column(k))

    @pl.when(early)
    def _():
        for k in range(2, DEPTH):
            greet((me, (z + k) % DEPTH))

    def time_link(t):
        return tl[0, :, :, t], tl[1, :, :, t]

    def space_link(mu, t):
        return sl[mu, 0, :, :, t], sl[mu, 1, :, :, t]

    def remote(src, dst, send, recv, device):
        return pltpu.make_async_remote_copy(
            src_ref=src, dst_ref=dst, send_sem=send, recv_sem=recv,
            device_id=device, device_id_type=MESH,
        )

    drain(sl, load_space)
    late_below = jnp.logical_or(z == 0, z > EARLY).astype(jnp.int32)
    of_height = jnp.where(early, EARLY - 1, EARLY)
    pl.semaphore_wait(barrier, ROWS - 1 + 2 + of_height + late_below)

    halos = []
    for mu in range(2):
        for c in range(2):
            halos.append(remote(
                sl.at[mu, :, :, :, :, pl.ds(c * PLANES, 1), :],
                space_halo.at[mu, :, :, :, :, pl.ds(HALO_ROWS[c], 1), :],
                halo_send, halo_recv, (me, below),
            ))
    for copy in halos:
        copy.start()

    drain(tl, load_time)
    prod = mul(time_link(0), time_link(1))
    total[0], total[1] = prod

    first = []
    for k in range(1, ROWS):
        first.append(remote(
            row_of(total, (member + k) % ROWS), row_of(in1, member),
            send1, recv1, in_row(k),
        ))
    for copy in first:
        copy.start()
    time_halos = []
    for c in range(2):
        time_halos.append(remote(
            tl.at[:, :, :, 0, pl.ds(c * PLANES, 1), :],
            time_halo.at[:, :, :, pl.ds(HALO_ROWS[c], 1), :],
            time_send, time_recv, (me, below),
        ))
    for copy in time_halos:
        copy.start()

    def tell_rows(sem, distance):
        for k in (distance, ROWS - distance):
            pl.semaphore_signal(sem, inc=1, device_id=in_column(k), device_id_type=MESH)

    tell_rows(near_sem, 1)

    rows = rows_of((ROWS, LANES))
    lanes = lanes_of((ROWS, LANES))
    top = rows % PLANES == PLANES - 1
    traces = []
    for t in range(2):
        ux, uy, uz = (space_link(mu, t) for mu in range(3))
        trace = overlap(mul(ux, ahead_x(uy)), mul(uy, ahead_y(ux)))
        for mu, along, ahead in ((0, ux, ahead_x), (1, uy, ahead_y)):
            rest = dagger_mul(uz, mul(along, ahead(uz)))
            around[mu, 0, :, :, t], around[mu, 1, :, :, t] = rest
            trace = trace + jnp.where(top, 0.0, overlap(rest, up_z(along)))
        traces.append(trace)

    pl.semaphore_wait(near_sem, 2)
    tell_rows(far_sem, 2)

    drain(space_halo.at[:, :, :, :, :, pl.ds(0, 2), :], halo_recv)
    densities = []
    for t in range(2):
        trace = traces[t]
        for mu in range(2):
            rest = around[mu, 0, :, :, t], around[mu, 1, :, :, t]
            beyond = space_halo[mu, 0, :, :, t], space_halo[mu, 1, :, :, t]
            trace = trace + jnp.where(top, overlap(rest, beyond), 0.0)
        densities.append(3.0 - trace * (1.0 / 3.0))

    def spread_sum(v):
        return jnp.broadcast_to(jnp.sum(v, axis=0, keepdims=True), (ROWS, LANES))

    part[0] = spread_sum(densities[0] + densities[1])

    def to_early(height):
        return remote(
            part.at[0, pl.ds(0, 1), :], part_z.at[pl.ds(z, 1), :],
            send_z, recv_z, (me, height),
        )

    for height in range(EARLY):
        @pl.when(z != height)
        def _(height=height):
            to_early(height).start()

    for t in range(2):
        of_row = jnp.sum(densities[t], axis=1, keepdims=True)
        spots = jnp.where(lanes == rows % PLANES, of_row, 0.0)
        profile = jnp.sum(spots, axis=0, keepdims=True) * (1.0 / (3 * 2 * LANES))
        small[t : t + 1, :] = profile

    drain(rows_in(in1, ROWS - 1), recv1)
    scan = pick(rows == member, load(total), load(in1))
    for s in (1, 2, 4):
        earlier = both(lambda v: pltpu.roll(v, s, 2), scan)
        scan = pick(rows >= s, mul(earlier, scan), scan)
    scanned[0], scanned[1] = scan

    def to_later(k):
        return remote(
            row_of(scanned, ROWS - 1), row_of(in2, group),
            send2, recv2, in_column(k),
        )

    pl.semaphore_wait(far_sem, 2)

    @pl.when(early)
    def _():
        for k in range(1, ROWS):
            pl.semaphore_signal(plane_sem, inc=1, device_id=in_row(k), device_id_type=MESH)

    for k in range(ROWS - 1, 0, -1):
        @pl.when(group + k < ROWS)
        def _(k=k):
            to_later(k).start()

    inside = or_unit(rows >= 1, both(lambda v: pltpu.roll(v, 1, 2), scan))
    for k in range(1, ROWS):
        @pl.when(group == k)
        def _(k=k):
            drain(rows_in(in2, k), recv2)
    before = or_unit(rows < group, load(in2))
    for s in (1, 2, 4):
        before = mul(before, both(lambda v: pltpu.roll(v, ROWS - s, 2), before))
    before = both(lambda v: jnp.broadcast_to(v[:, :, 0:1], v.shape), before)
    spread[0], spread[1] = mul(before, inside)

    def return_carries():
        for k in range(1, ROWS):
            remote(
                row_of(spread, (member + k) % ROWS), row_of(carry, member),
                send3, recv3, in_row(k),
            ).start()

    ahead = group < ROWS // 2

    @pl.when(ahead)
    def _():
        return_carries()

    def to_plane(row, k):
        return remote(
            part.at[1, pl.ds(0, 1), :], part_all.at[group, pl.ds(member, 1), :],
            send_all, recv_all, (row * ROWS + (member + k) % ROWS, z),
        )

    @pl.when(early)
    def _():
        drain(part_z.at[pl.ds(0, DEPTH - 1), :], recv_z)
        part[1] = spread_sum(jnp.where(rows == z, part[0], part_z[...]))
        pl.semaphore_wait(plane_sem, ROWS - 1)
        for row in range(ROWS):
            @pl.when(row != group)
            def _(row=row):
                to_plane(row, 0).start()

            for k in range(1, ROWS):
                to_plane(row, k).start()

    @pl.when(jnp.logical_not(ahead))
    def _():
        return_carries()

    drain(rows_in(carry, ROWS - 1), recv3)
    g0 = pick(rows == member, load(spread), load(carry))
    g1 = mul(g0, time_link(0))
    g = (g0, g1)
    for t in range(2):
        g_out[0, :, :, t], g_out[1, :, :, t] = g[t]
    for c in range(2):
        remote(
            g_out.at[:, :, :, 0, pl.ds(c * PLANES, 1), :],
            carry_halo.at[:, :, :, pl.ds(HALO_ROWS[c], 1), :],
            send4, recv4, (me, below),
        ).start()

    def fix(mu, t, ahead):
        v = mul_dagger(mul(g[t], space_link(mu, t)), ahead)
        v_out[mu, 0, :, :, t], v_out[mu, 1, :, :, t] = v

    for t in range(2):
        fix(0, t, ahead_x(g[t]))
    for t in range(2):
        fix(1, t, ahead_y(g[t]))
    drain(rows_in(time_halo, 2), time_recv)
    drain(rows_in(carry_halo, 2), recv4)
    g0z = ahead_z(g0, load(carry_halo))
    g1z = mul(g0z, ahead_z(time_link(0), load(time_halo)))
    for t, ahead in ((0, g0z), (1, g1z)):
        fix(2, t, ahead)

    plane_rows = in1.at[pl.ds(0, 1), :, :, pl.ds(0, ROWS - 1), :]

    def to_late(height):
        return remote(part.at[2], part_back, send_back, recv_back, (me, height))

    def tell_late(act):
        @pl.when(z == EARLY - 1)
        def _():
            for height in range(EARLY, DEPTH - 1):
                act(to_late(height))

        @pl.when(z == EARLY - 2)
        def _():
            act(to_late(DEPTH - 1))

    def write_mean(sites):
        mean = jnp.sum(sites[0:1], axis=1, keepdims=True)
        small[2:3, :] = jnp.broadcast_to(mean * (1.0 / (3 * 2 * LANES * 4096)), (1, LANES))

    @pl.when(early)
    def _():
        drain(plane_rows, recv_all)
        parts = None
        for k in range(ROWS):
            mine = jnp.logical_and(rows == member, group == k)
            got = jnp.where(mine, part[1], part_all[k])
            parts = got if parts is None else parts + got
        whole = spread_sum(parts)
        part[2] = whole
        tell_late(lambda copy: copy.start())
        write_mean(whole)
        drain(plane_rows, send_all)
        drain(part.at[0, pl.ds(0, EARLY - 1), :], send_z)

    @pl.when(jnp.logical_not(early))
    def _():
        drain(part_back, recv_back)
        write_mean(part_back[...])
        drain(part.at[0, pl.ds(0, EARLY), :], send_z)

    drain(space_halo.at[:, :, :, :, :, pl.ds(0, 2), :], halo_send)
    drain(rows_in(time_halo, 2), time_send)
    drain(rows_in(in1, ROWS - 1), send1)
    drain(rows_in(carry, ROWS - 1), send3)
    for k in range(1, ROWS):
        @pl.when(group == ROWS - 1 - k)
        def _(k=k):
            drain(rows_in(in2, k), send2)

    drain(rows_in(carry_halo, 2), send4)

    @pl.when(z == EARLY - 1)
    def _():
        drain(part, send_back)

    @pl.when(z == EARLY - 2)
    def _():
        drain(part_back, send_back)


def write_out(
    g_out, v_out, small, gauge_ref, fixed_ref, profile_ref, mean_ref, profile, mean, sem
):
    profile[...] = small[0:2, :PLANES]
    mean[...] = small[2:3, 0:1]
    copies = []
    for c in range(2):
        planes, lanes = pl.ds(c * PLANES, PLANES), pl.ds(c * LANES, LANES)
        for src, dst in (
            (v_out.at[:, :, :, :, :, planes, :], fixed_ref.at[:, :, :, :, :, :, lanes]),
            (g_out.at[:, :, :, :, planes, :], gauge_ref.at[:, :, :, :, :, lanes]),
        ):
            copies.append(pltpu.make_async_copy(src, dst, sem.at[len(copies)]))
    for src, dst in ((profile, profile_ref), (mean, mean_ref)):
        copies.append(pltpu.make_async_copy(src, dst, sem.at[len(copies)]))
    for copy in copies:
        copy.start()
    for copy in copies:
        copy.wait()


def on_device(time_links, space_links):
    pair = (2, 3, 3, ROWS, LANES)
    vmem = pl.BlockSpec(memory_space=pltpu.VMEM)
    anywhere = pl.BlockSpec(memory_space=pl.ANY)
    staged = pl.pallas_call(
        kernel,
        out_shape=(
            pltpu.VMEM((2, 3, 3, 2, ROWS, LANES), F32),
            pltpu.VMEM((3, 2, 3, 3, 2, ROWS, LANES), F32),
            pltpu.VMEM((ROWS, LANES), F32),
        ),
        in_specs=[pl.BlockSpec(memory_space=pltpu.HBM)] * 2,
        out_specs=(vmem,) * 3,
        scratch_shapes=[
            pltpu.VMEM((2, 3, 3, 2, ROWS, LANES), F32),
            pltpu.VMEM((3, 2, 3, 3, 2, ROWS, LANES), F32),
            *[pltpu.VMEM(pair, F32)] * 8,
            pltpu.VMEM((2, 2, 3, 3, 2, ROWS, LANES), F32),
            pltpu.VMEM((2, 2, 3, 3, 2, ROWS, LANES), F32),
            pltpu.VMEM((3, ROWS, LANES), F32),
            pltpu.VMEM((ROWS, LANES), F32),
            pltpu.VMEM((ROWS, ROWS, LANES), F32),
            pltpu.VMEM((ROWS, LANES), F32),
            pltpu.SemaphoreType.DMA((SEMAPHORES,)),
            *[pltpu.SemaphoreType.REGULAR] * 3,
        ],
        compiler_params=pltpu.CompilerParams(collective_id=0, has_side_effects=True),
    )(time_links, space_links)
    gauge, fixed, profile, mean = pl.pallas_call(
        write_out,
        out_shape=(
            jax.ShapeDtypeStruct(time_links.shape, F32),
            jax.ShapeDtypeStruct(space_links.shape, F32),
            jax.ShapeDtypeStruct((2, PLANES), F32),
            jax.ShapeDtypeStruct((1, 1), F32),
        ),
        in_specs=[vmem] * 3,
        out_specs=(anywhere,) * 4,
        scratch_shapes=[
            pltpu.VMEM((2, PLANES), F32), pltpu.VMEM((1, 1), F32), pltpu.SemaphoreType.DMA((6,)),
        ],
        compiler_params=pltpu.CompilerParams(vmem_limit_bytes=4 * 2**20),
    )(*staged)
    return gauge, fixed, profile, mean.reshape(())


def solution(mesh):
    placed = (P(None, None, None, "ta", "gz", None), P(None, None, None, None, "ta", "gz", None))
    return jax.shard_map(
        on_device,
        mesh=mesh,
        in_specs=placed,
        out_specs=(*placed, P("ta", "gz"), P()),
        check_vma=False,
    )
```
